32 devices in a mesh: rep: 2 (over z, core), dp: 16 (over x, y).
Axes of the slice: x: 4, y: 4, z: 1, core: 2. Of those that a mesh axis runs over, the one named last changes fastest.
The devices are a block of a 4x4x8 slice.
Arguments:
- x: bfloat16 [32, 4096, 640], P(('rep', 'dp')), parts along dimension 0
- dy: bfloat16 [32, 4096, 640], P(('rep', 'dp')), parts along dimension 0
- w_gate: bfloat16 [2, 640, 3200], P(None, 'dp')
- w_up: bfloat16 [2, 640, 3200], P(None, 'dp')
- w_down: bfloat16 [2, 3200, 640], P(None, 'dp')
- m_w_gate: float32 [2, 640, 3200], P(None, 'dp')
- m_w_up: float32 [2, 640, 3200], P(None, 'dp')
- m_w_down: float32 [2, 3200, 640], P(None, 'dp')
- v_w_gate: float32 [2, 640, 3200], P(None, 'dp')
- v_w_up: float32 [2, 640, 3200], P(None, 'dp')
- v_w_down: float32 [2, 3200, 640], P(None, 'dp')
Outputs:
- output 1: bfloat16 [4, 640, 3200], P('rep', 'dp'), parts along dimension 0
- output 2: bfloat16 [4, 640, 3200], P('rep', 'dp'), parts along dimension 0
- output 3: bfloat16 [4, 3200, 640], P('rep', 'dp'), parts along dimension 0
- output 4: float32 [4, 640, 3200], P('rep', 'dp'), parts along dimension 0
- output 5: float32 [4, 640, 3200], P('rep', 'dp'), parts along dimension 0
- output 6: float32 [4, 3200, 640], P('rep', 'dp'), parts along dimension 0
- output 7: float32 [4, 640, 3200], P('rep', 'dp'), parts along dimension 0
- output 8: float32 [4, 640, 3200], P('rep', 'dp'), parts along dimension 0
- output 9: float32 [4, 3200, 640], P('rep', 'dp'), parts along dimension 0
There are 2 independent parts. The reference program is written for one: setup_inputs(seed, part) draws one part's arguments, and reference() takes and returns one part's arrays. A program takes and returns all parts, laid end to end along the dimension named above; an argument that names none is the same for every part.
All inputs are finite; a program needn't handle non-finite values.
Results may differ from the reference program's by a relative error of at most 0.022.
Values are sent between devices in bfloat16 or wider.
A program may use at most 768 MiB of HBM per device.

```python
import jax
import jax.numpy as jnp
from jax import lax

SEQUENCES = 16
TOKENS = 4096
D = 640
FF = 3200
LAYERS = 2
NAMES = ("w_gate", "w_up", "w_down")
SHAPES = {"w_gate": (LAYERS, D, FF), "w_up": (LAYERS, D, FF), "w_down": (LAYERS, FF, D)}


def bump(key, n, height):
    away = (jnp.arange(n, dtype=jnp.int32) - jax.random.randint(key, (), 0, n, jnp.int32)) % n
    return jnp.where(away < n // 8, height, 1.0)


def together(key, own, strength):
    shared = jax.random.normal(key, own.shape[1:], jnp.float32)
    return (own + strength * shared) * lax.rsqrt(1 + strength * strength)


def setup_inputs(seed: int = 0, part: int = 0) -> dict:
    kx, kdy, ka, kb, kz, kf, kh, kl, *keys = jax.random.split(jax.random.key(seed), 8 + 3 * len(NAMES))
    kx, kdy, ka, kb = (jax.random.fold_in(k, part) for k in (kx, kdy, ka, kb))
    kw, km, kv = (keys[i::3] for i in range(3))
    shape = (SEQUENCES, TOKENS, D)
    much_x, much_dy = jax.random.uniform(kz, (2,), jnp.float32, 0.0, 1.0)
    loud = 2.0 ** jax.random.uniform(jax.random.fold_in(kz, 1), (), jnp.float32, -1.0, 2.0)
    layers = 2.0 ** jax.random.uniform(kl, (LAYERS, 1, 1), jnp.float32, -1.0, 1.0)
    x = together(ka, jax.random.normal(kx, shape, jnp.float32), much_x) * bump(kf, D, 4.0)
    dy = together(kb, jax.random.normal(kdy, shape, jnp.float32), much_dy)
    drawn = {"x": x.astype(jnp.bfloat16), "dy": (loud * dy * (SEQUENCES * TOKENS) ** -0.5).astype(jnp.bfloat16)}
    for key, name in zip(kw, NAMES, strict=True):
        w = jax.random.normal(key, SHAPES[name], jnp.float32) * SHAPES[name][1] ** -0.5
        drawn[name] = (w * {"w_gate": 1.0, "w_up": bump(kh, FF, 4.0), "w_down": layers}[name]).astype(jnp.bfloat16)
    for key, name in zip(km, NAMES, strict=True):
        drawn[f"m_{name}"] = 0.1 * jax.random.normal(key, SHAPES[name], jnp.float32)
    for key, name in zip(kv, NAMES, strict=True):
        drawn[f"v_{name}"] = jax.random.uniform(key, SHAPES[name], jnp.float32, 0.005, 0.015)
    return drawn


def matmul(a, w):
    return jnp.dot(a, w, preferred_element_type=jnp.float32).astype(jnp.bfloat16)


def normed(h):
    wide = h.astype(jnp.float32)
    scale = lax.rsqrt(jnp.mean(wide**2, -1, keepdims=True) + 1e-6)
    return (wide * scale).astype(jnp.bfloat16)


def layer(h, w):
    a = normed(h)
    gate = jnp.dot(a, w["w_gate"], preferred_element_type=jnp.float32)
    up = jnp.dot(a, w["w_up"], preferred_element_type=jnp.float32)
    return h + matmul((jax.nn.silu(gate) * up).astype(jnp.bfloat16), w["w_down"])


def adamw(w, m, v, g):
    m = 0.9 * m + 0.1 * g
    v = 0.95 * v + 0.05 * g * g
    step = m * lax.rsqrt(v + 1e-8) + 0.1 * w
    return (w - 0.02 * step).astype(jnp.bfloat16), m, v


def clipped(gradients, sum_of_squares, count):
    factor = jnp.minimum(1.0, 0.5 * lax.rsqrt(sum_of_squares / count + 1e-30))
    return [g * factor for g in gradients]


def stack(weights, h):
    return lax.scan(lambda h, w: (layer(h, w), None), h, weights)[0]


def reference(x, dy, w_gate, w_up, w_down, m_w_gate, m_w_up, m_w_down, v_w_gate, v_w_up, v_w_down):
    weights = dict(zip(NAMES, (w_gate, w_up, w_down), strict=True))

    def take(so_far, sequence):
        h, by_y = sequence
        _, back = jax.vjp(lambda w: stack(w, h), weights)
        return jax.tree.map(lambda total, term: total + term.astype(jnp.float32), so_far, back(by_y)[0]), None

    none_yet = {name: jnp.zeros(w.shape, jnp.float32) for name, w in weights.items()}
    by_weights, _ = lax.scan(take, none_yet, (x, dy))
    gradients = [by_weights[name].astype(jnp.bfloat16).astype(jnp.float32) for name in NAMES]
    gradients = clipped(gradients, sum(jnp.sum(g * g) for g in gradients), sum(g.size for g in gradients))
    new = [
        adamw(w.astype(jnp.float32), m, v, g)
        for w, m, v, g in zip((w_gate, w_up, w_down), (m_w_gate, m_w_up, m_w_down), (v_w_gate, v_w_up, v_w_down), gradients, strict=True)
    ]
    return tuple(one[which] for which in range(3) for one in new)
```

```python
import functools
import math

import jax
import jax.numpy as jnp
from jax import lax
from jax.experimental import pallas as pl
from jax.experimental.pallas import tpu as pltpu
from jax.sharding import PartitionSpec as P

BF, F32 = jnp.bfloat16, jnp.float32
LANES = 128
VMEM = 67000000


def place(side):
    me = lax.axis_index("dp")
    x, y = me // side, me % side
    on, back = (x + 1) % side, (x + side - 1) % side
    up, down = (y + 1) % side, (y + side - 1) % side
    return x, y, {"x": (on * side + y, back * side + y), "y": (x * side + up, x * side + down)}


def greet(near):
    barrier = pltpu.get_barrier_semaphore()
    for pair in near.values():
        for other in pair:
            pl.semaphore_signal(barrier, inc=1, device_id={"dp": other}, device_id_type=pl.DeviceIdType.MESH)
    pl.semaphore_wait(barrier, 4)


def remote(src, dst, sems, number, to):
    return pltpu.make_async_remote_copy(
        src_ref=src, dst_ref=dst, send_sem=sems[0].at[number], recv_sem=sems[1].at[number], device_id={"dp": to}, device_id_type=pl.DeviceIdType.MESH
    )


def half(n):
    return (n // LANES + 1) // 2 * LANES


def all_gather_events(side, shards, whole, sems, local):
    x, y, near = place(side)
    cut = (shards[2].shape[0] + 1) // 2
    flows = []
    for k in range(2):
        ref = whole[k]
        flows.append(("xy"[k], shards[k], lambda i, j, ref=ref: ref.at[i, j]))
    for k, (lo, n) in enumerate(((0, cut), (cut, shards[2].shape[0] - cut))):
        flows.append(("xy"[k], shards[2].at[pl.ds(lo, n)], lambda i, j, lo=lo, n=n: whole[2].at[pl.ds(lo, n), i, j]))
    every = pl.ds(0, side)

    def copies(step):
        out = []
        for k, (first, mine, at) in enumerate(flows):
            second = "y" if first == "x" else "x"
            c1, c2 = (x, y) if first == "x" else (y, x)

            def spot(a, b, at=at, first=first):
                return at(a, b) if first == "x" else at(b, a)

            lanes = mine.shape[-1]
            cut_at = half(lanes)
            if step == 0:
                pairs = [(near[first][i], mine, spot(c1, c2)) for i in range(2)]
            elif step == 1:
                pairs = []
                for i, (lo, n) in enumerate(((0, cut_at), (cut_at, lanes - cut_at))):
                    origin = (c1 + (side - 1 if i == 0 else 1)) % side
                    ref = spot(origin, c2)
                    part = ref.at[(slice(None),) * (len(ref.shape) - 1) + (pl.ds(lo, n),)]
                    pairs.append((near[first][i], part, part))
            elif step == 2:
                pairs = [(near[second][i], spot(every, c2), spot(every, c2)) for i in range(2)]
            else:
                pairs = []
                for i in range(2):
                    origin = (c2 + (side - 1 if i == 0 else 1)) % side
                    ref = spot(pl.ds(i * (side // 2), side // 2), origin)
                    pairs.append((near[second][i], ref, ref))
            for i, (to, src, dst) in enumerate(pairs):
                out.append(remote(src, dst, sems, (k * 4 + step) * 2 + i, to))
        return out

    own = [pltpu.make_async_copy(mine, at(x, y), local.at[k]) for k, (_, mine, at) in enumerate(flows)]

    def begin():
        greet(near)
        for c in own:
            c.start()
        for c in copies(0):
            c.start()

    def middle(step):
        for c in copies(step - 1):
            c.wait_recv()
        if step == 2:
            for c in own:
                c.wait()
        for c in copies(step):
            c.start()

    def finish():
        for c in copies(3):
            c.wait_recv()
        for step in range(4):
            for c in copies(step):
                c.wait_send()

    return [begin, functools.partial(middle, 1), functools.partial(middle, 2), functools.partial(middle, 3), finish]


AG_SEMS = [pltpu.SemaphoreType.DMA((32,)), pltpu.SemaphoreType.DMA((32,)), pltpu.SemaphoreType.DMA((4,))]


def gathered_shapes(side, shards):
    up, down = shards[0], shards[2]
    wide = jax.ShapeDtypeStruct((side, side) + up.shape, BF)
    return [wide, wide, jax.ShapeDtypeStruct((down.shape[0], side, side) + down.shape[1:], BF)]


def flat(whole):
    gate, up, down = whole
    d = gate.shape[0] * gate.shape[1] * gate.shape[2]
    return gate.reshape(d, -1), up.reshape(d, -1), down.reshape(-1, down.shape[-1])


def gather_kernel(side, *refs):
    shards, whole, (send, recv, local) = refs[:3], refs[3:6], refs[6:]
    for event in all_gather_events(side, shards, whole, (send, recv), local):
        event()


def gather(side, shards):
    return pl.pallas_call(
        functools.partial(gather_kernel, side),
        out_shape=gathered_shapes(side, shards),
        in_specs=[pl.BlockSpec(memory_space=pl.ANY)] * 3,
        out_specs=[pl.BlockSpec(memory_space=pl.ANY)] * 3,
        scratch_shapes=AG_SEMS,
        compiler_params=pltpu.CompilerParams(collective_id=0, has_side_effects=True),
        name="gather",
    )(*shards)


def norm(h):
    wide = h.astype(F32)
    scale = lax.rsqrt(jnp.mean(wide * wide, -1, keepdims=True) + 1e-6)
    return wide, scale


def dot(a, b, dims=((1,), (0,))):
    return lax.dot_general(a, b, (dims, ((), ())), preferred_element_type=F32)


def forward_kernel(side, steps, when, *refs):
    h_ref, wg, wu, wd = refs[:4]
    shards, out_ref, whole = refs[4:7], refs[7], refs[8:11]
    acc, (send, recv, local) = refs[11], refs[12:]
    t = pl.program_id(0)
    events = all_gather_events(side, shards, whole, (send, recv), local)
    for event, at in zip(events[:-1], when):
        pl.when(t == at)(event)
    wide, scale = norm(h_ref[...])
    a = (wide * scale).astype(BF)
    d, ff = wg.shape
    for j in range(ff // d):
        cols = pl.ds(j * d, d)
        gate, up = dot(a, wg[:, cols]), dot(a, wu[:, cols])
        act = (gate * jax.nn.sigmoid(gate) * up).astype(BF)
        term = dot(act, wd[cols, :])
        if j == 0:
            acc[...] = term
        else:
            acc[...] += term
    out_ref[...] = h_ref[...] + acc[...].astype(BF)
    pl.when(t == steps - 1)(events[-1])


def forward(side, h, weights, shards):
    tokens, d = h.shape
    steps = 16
    tile = tokens // steps
    ff = weights[0].shape[1]
    any_ = pl.BlockSpec(memory_space=pl.ANY)
    resident = [pl.BlockSpec(w.shape, lambda t: (0, 0)) for w in weights]
    rows = pl.BlockSpec((tile, d), lambda t: (t, 0))
    out = pl.pallas_call(
        functools.partial(forward_kernel, side, steps, (0, 3, 5, 14)),
        grid=(steps,),
        out_shape=[jax.ShapeDtypeStruct(h.shape, BF)] + gathered_shapes(side, shards),
        in_specs=[rows] + resident + [any_] * 3,
        out_specs=[rows] + [any_] * 3,
        scratch_shapes=[pltpu.VMEM((tile, d), F32)] + AG_SEMS,
        compiler_params=pltpu.CompilerParams(collective_id=1, has_side_effects=True, vmem_limit_bytes=VMEM, dimension_semantics=("arbitrary",)),
        cost_estimate=pl.CostEstimate(flops=6 * tokens * d * ff, bytes_accessed=20 * tokens * d, transcendentals=tokens * ff),
        name="forward",
    )(h, *weights, *shards)
    return out[0], out[1:]


def scatter_events(side, terms, bufs, sems, out_ref):
    x, y, near = place(side)
    r1, r2, s2, total, t2, q1a, q1b, q2, s4 = bufs
    lanes = terms.shape[-1]
    lo = half(lanes)
    part = (pl.ds(0, lo), pl.ds(lo, lanes - lo))
    h = side // 2

    def parts(k):
        first = "y" if k != 1 else "x"
        c1, c2 = (y, x) if first == "y" else (x, y)

        def at(a, b):
            return terms.at[k, b, a] if first == "y" else terms.at[k, a, b]

        return near[first], near["x" if first == "y" else "y"], c1, c2, at

    def copies(step):
        out = []
        for k in range(3):
            first, second, c1, c2, at = parts(k)
            if step == 0:
                far = (c1 + 2) % side
                pairs = [(first[i], at(far, pl.ds(i * h, h)), r1.at[k, i]) for i in range(2)]
            elif step == 1:
                pairs = [(first[i], s2.at[k, i], r2.at[k, i]) for i in range(2)]
            elif step == 2:
                pairs = [(second[i], t2.at[k, :, part[i]], (q1a, q1b)[i].at[k]) for i in range(2)]
            else:
                pairs = [(second[i], s4.at[k, i], q2.at[k, i]) for i in range(2)]
            for i, (to, src, dst) in enumerate(pairs):
                out.append(remote(src, dst, sems, (k * 4 + step) * 2 + i, to))
        return out

    def wide(ref):
        return ref[...].astype(F32)

    def zero():
        for c in copies(0):
            c.start()

    def one():
        for c in copies(0):
            c.wait_recv()
        for k in range(3):
            _, _, c1, c2, at = parts(k)
            for i in range(2):
                dest = (c1 + (1 if i == 0 else side - 1)) % side
                for b in range(side):
                    mine = at(dest, b)
                    if b // h == i:
                        s2[k, i, b] = (wide(mine) + wide(r1.at[k, i, b - i * h])).astype(BF)
                    else:
                        s2[k, i, b] = mine[...]
        for c in copies(1):
            c.start()

    def two():
        for c in copies(1):
            c.wait_recv()
        for k in range(3):
            _, _, c1, c2, at = parts(k)
            for b in range(side):
                total[k, b] = wide(at(c1, b)) + wide(r2.at[k, 0, b]) + wide(r2.at[k, 1, b])
            t2[k] = total[k, (c2 + 2) % side].astype(BF)
        for c in copies(2):
            c.start()

    def three():
        for c in copies(2):
            c.wait_recv()
        for k in range(3):
            _, _, c1, c2, at = parts(k)
            on, back = (c2 + 1) % side, (c2 + side - 1) % side
            s4[k, 0, :, part[0]] = (total[k, on, :, part[0]] + wide(q1a.at[k])).astype(BF)
            s4[k, 0, :, part[1]] = total[k, on, :, part[1]].astype(BF)
            s4[k, 1, :, part[0]] = total[k, back, :, part[0]].astype(BF)
            s4[k, 1, :, part[1]] = (total[k, back, :, part[1]] + wide(q1b.at[k])).astype(BF)
        for c in copies(3):
            c.start()

    def four(chunk):
        for c in copies(3):
            c.wait_recv()
        for k in range(3):
            _, _, c1, c2, at = parts(k)
            out_ref[chunk, k] = (total[k, c2] + wide(q2.at[k, 0]) + wide(q2.at[k, 1])).astype(BF)
        for step in range(4):
            for c in copies(step):
                c.wait_send()

    return near, (zero, one, two, three, four)


def scatter_scratch(side, rows, lanes):
    lo = half(lanes)
    return [
        pltpu.VMEM((3, 2, side // 2, rows, lanes), BF),
        pltpu.VMEM((3, 2, side, rows, lanes), BF),
        pltpu.VMEM((3, 2, side, rows, lanes), BF),
        pltpu.VMEM((3, side, rows, lanes), F32),
        pltpu.VMEM((3, rows, lanes), BF),
        pltpu.VMEM((3, rows, lo), BF),
        pltpu.VMEM((3, rows, lanes - lo), BF),
        pltpu.VMEM((3, 2, rows, lanes), BF),
        pltpu.VMEM((3, 2, rows, lanes), BF),
    ]


def backward_kernel(side, chunks, steps, when, inner, *refs):
    h_ref, by_ref, wg, wu, wd = refs[:5]
    refs = refs[5:]
    if inner:
        out_ref, by_out, refs = refs[0], refs[1], refs[2:]
        by_a, refs = refs[0], refs[1:]
    else:
        out_ref, refs = refs[0], refs[1:]
    a_s, at_s, byt_s, acc_g, acc_u, acc_d, terms = refs[:7]
    bufs, sems = refs[7:16], refs[16:18]
    j, t = pl.program_id(0), pl.program_id(1)
    tile, d = h_ref.shape
    rows = terms.shape[3]
    near, (zero, one, two, three, four) = scatter_events(side, terms, bufs, sems, out_ref)
    pl.when((j == 0) & (t == 0))(lambda: greet(near))
    later = j > 0
    pl.when(later & (t == when[0]))(zero)
    pl.when(later & (t == when[1]))(one)
    pl.when(later & (t == when[2]))(two)
    pl.when(later & (t == when[3]))(three)
    pl.when(later & (t == when[4]))(lambda: four(j - 1))

    here = pl.ds(pl.multiple_of(t * tile, tile), tile)

    @pl.when(j == 0)
    def _():
        wide, scale = norm(h_ref[...])
        a = wide * scale
        a_s[here, :] = a.astype(BF)
        at_s[t] = a.T.astype(BF)
        byt_s[t] = by_ref[...].astype(F32).T.astype(BF)

    a, by = a_s[here, :], by_ref[...]
    gate, up = dot(a, wg[...]), dot(a, wu[...])
    by_act = dot(by, wd[...], ((1,), (1,))).astype(BF).astype(F32)
    sig = jax.nn.sigmoid(gate)
    silu = gate * sig
    act = (silu * up).astype(BF)
    by_up = (by_act * silu).astype(BF)
    by_gate = (by_act * up * (sig + silu * (1.0 - sig))).astype(BF)
    at, byt = at_s[t], byt_s[t]
    new = (dot(at, by_gate), dot(at, by_up), dot(byt, act))

    @pl.when(t == 0)
    def _():
        for acc, term in zip((acc_g, acc_u, acc_d), new):
            acc[...] = term

    @pl.when(t > 0)
    def _():
        for acc, term in zip((acc_g, acc_u, acc_d), new):
            acc[...] += term

    if inner:
        term = dot(by_gate, wg[...], ((1,), (1,))) + dot(by_up, wu[...], ((1,), (1,)))

        @pl.when(j == 0)
        def _():
            by_a[here, :] = term

        @pl.when(j > 0)
        def _():
            by_a[here, :] += term

        @pl.when(j == chunks - 1)
        def _():
            g = by_a[here, :].astype(BF).astype(F32)
            wide, scale = norm(h_ref[...])
            inside = jnp.mean(g * wide, -1, keepdims=True)
            back = scale * g - (scale * scale * scale * inside) * wide
            by_out[...] = by_ref[...] + back.astype(BF)

    @pl.when(t == steps - 1)
    def _():
        for k, acc in enumerate((acc_g, acc_u)):
            for i in range(side):
                for n in range(side):
                    terms[k, i, n] = acc[pl.ds((i * side + n) * rows, rows), :].astype(BF)
        acc_d[...] = acc_d[...].T
        for i in range(side):
            for n in range(side):
                terms[2, i, n] = acc_d[pl.ds((i * side + n) * rows, rows), :].astype(BF)

    @pl.when((j == chunks - 1) & (t == steps - 1))
    def _():
        zero()
        one()
        two()
        three()
        four(chunks - 1)


def backward(side, h, by, weights, inner, number):
    tokens, d = h.shape
    ff = weights[0].shape[1]
    chunks, steps = ff // d, 8
    tile, rows = tokens // steps, d // side // side
    stream = pl.BlockSpec((tile, d), lambda j, t: (t, 0))
    out_shape = [jax.ShapeDtypeStruct((chunks, 3, rows, d), BF)]
    out_specs = [pl.BlockSpec((chunks, 3, rows, d), lambda j, t: (0, 0, 0, 0))]
    scratch = []
    if inner:
        out_shape.append(jax.ShapeDtypeStruct(h.shape, BF))
        out_specs.append(pl.BlockSpec((tile, d), lambda j, t: (jnp.where(j == chunks - 1, t, 0), 0)))
        scratch.append(pltpu.VMEM((tokens, d), F32))
    scratch += [pltpu.VMEM((tokens, d), BF), pltpu.VMEM((steps, d, tile), BF), pltpu.VMEM((steps, d, tile), BF)]
    scratch += [pltpu.VMEM((d, d), F32)] * 3 + [pltpu.VMEM((3, side, side, rows, d), BF)]
    scratch += scatter_scratch(side, rows, d) + [pltpu.SemaphoreType.DMA((24,)), pltpu.SemaphoreType.DMA((24,))]
    return pl.pallas_call(
        functools.partial(backward_kernel, side, chunks, steps, (0, 2, 5, 6, 7), inner),
        grid=(chunks, steps),
        out_shape=out_shape,
        in_specs=[stream, stream]
        + [pl.BlockSpec((d, d), lambda j, t: (0, j))] * 2
        + [pl.BlockSpec((d, d), lambda j, t: (j, 0))],
        out_specs=out_specs,
        scratch_shapes=scratch,
        compiler_params=pltpu.CompilerParams(
            collective_id=number, has_side_effects=True, vmem_limit_bytes=VMEM, dimension_semantics=("arbitrary", "arbitrary")
        ),
        cost_estimate=pl.CostEstimate(flops=(16 if inner else 12) * tokens * d * ff, bytes_accessed=30 * tokens * d, transcendentals=tokens * ff),
        name="backward",
    )(h, by, *weights)


def total_kernel(side, part_ref, out_ref, got, held, send, recv):
    x, y, near = place(side)
    greet_all = [x * side + (y + s) % side for s in range(1, side)], [(x + s) % side * side + y for s in range(1, side)]
    barrier = pltpu.get_barrier_semaphore()
    for peers in greet_all:
        for other in peers:
            pl.semaphore_signal(barrier, inc=1, device_id={"dp": other}, device_id_type=pl.DeviceIdType.MESH)
    pl.semaphore_wait(barrier, 2 * (side - 1))
    held[0] = part_ref[...]
    for phase, peers in enumerate(greet_all):
        sent = [remote(held.at[phase], got.at[phase, s], (send.at[phase], recv.at[phase]), s, other) for s, other in enumerate(peers)]
        for c in sent:
            c.start()
        for c in sent:
            c.wait()
        sum_ = held[phase]
        for s in range(side - 1):
            sum_ = sum_ + got[phase, s]
        if phase == 0:
            held[1] = sum_
        else:
            out_ref[...] = sum_


def total(side, part):
    tile = (8, LANES)
    n = side - 1
    out = pl.pallas_call(
        functools.partial(total_kernel, side),
        out_shape=jax.ShapeDtypeStruct(tile, F32),
        in_specs=[pl.BlockSpec(memory_space=pltpu.VMEM)],
        out_specs=pl.BlockSpec(memory_space=pltpu.VMEM),
        scratch_shapes=[
            pltpu.VMEM((2, n) + tile, F32),
            pltpu.VMEM((2,) + tile, F32),
            pltpu.SemaphoreType.DMA((2, n)),
            pltpu.SemaphoreType.DMA((2, n)),
        ],
        compiler_params=pltpu.CompilerParams(collective_id=4, has_side_effects=True),
        name="total",
    )(jnp.broadcast_to(part, tile))
    return out[0, 0]


def adamw(w, m, v, g):
    m = 0.9 * m + 0.1 * g
    v = 0.95 * v + 0.05 * g * g
    step = m * lax.rsqrt(v + 1e-8) + 0.1 * w
    return (w - 0.02 * step).astype(BF), m, v


def solution(mesh):
    group = mesh.shape["dp"]
    side = math.isqrt(group)

    def step(x, dy, *arrays):
        weights, m, v = (arrays[i : i + 3] for i in (0, 3, 6))
        gate, up, down = weights
        layers, rows, ff = gate.shape
        d = rows * group
        chunks = ff // d
        spread = (layers, rows, group, chunks, rows)
        gate, up = (w.reshape(spread).swapaxes(2, 3).reshape(w.shape) for w in (gate, up))
        down = down.reshape(layers, chunks, rows, d)
        shards = [(gate[n], up[n], down[n]) for n in range(layers)]
        h, by = x[0], dy[0]
        kept = []
        whole = [flat(gather(side, shards[0]))]
        for number in range(layers - 1):
            kept.append(h)
            h, following = forward(side, h, whole[number], shards[number + 1])
            whole.append(flat(following))
        kept.append(h)
        mine = [None] * layers
        for number in reversed(range(layers)):
            out = backward(side, kept[number], by, whole[number], number > 0, 2 + min(number, 1))
            mine[number] = out[0]
            if number > 0:
                by = out[1]
        mine = jnp.stack(mine)
        squares = total(side, jnp.sum(mine.astype(F32) ** 2))
        count = group * mine.size
        factor = jnp.minimum(1.0, 0.5 * lax.rsqrt(squares / count + 1e-30))
        gradients = [mine[:, :, k].reshape(layers, chunks, rows, group, rows).transpose(0, 2, 3, 1, 4).reshape(layers, rows, ff) for k in range(2)]
        gradients.append(mine[:, :, 2].reshape(layers, chunks * rows, d))
        new = [adamw(w.astype(F32), m, v, g.astype(F32) * factor) for w, m, v, g in zip(weights, m, v, gradients, strict=True)]
        return tuple(one[which] for which in range(3) for one in new)

    states, cut = P(("rep", "dp"), None, None), P(None, "dp", None)
    return jax.shard_map(
        step,
        mesh=mesh,
        in_specs=(states, states) + (cut,) * 9,
        out_specs=(P("rep", "dp", None),) * 9,
        check_vma=False,
    )
```
